32 devices in a mesh: gx: 4 (over z), gy: 4 (over y, x), gz: 2 (over core).
Axes of the slice: x: 2, y: 2, z: 4, core: 2. Of those that a mesh axis runs over, the one named last changes fastest.
Arguments:
- positions: float32 [3, 64, 64, 512], P(None, 'gx', 'gy', 'gz'), may hold values from -6 to 6
- pair_node: int32 [4, 4, 2, 32, 256], P('gx', 'gy', 'gz'), may hold values from 0 to 255
- pair_line: int32 [4, 4, 2, 32], P('gx', 'gy', 'gz'), may hold values from 0 to 255
- pair_far: int32 [4, 4, 2, 32, 256], P('gx', 'gy', 'gz'), may hold values from 0 to 261, as said below
- far_line: int32 [4, 4, 2, 32], P('gx', 'gy', 'gz'), may hold values from 0 to 483, as said below
- pair_geom: float32 [4, 4, 2, 32, 4, 256], P('gx', 'gy', 'gz'), may hold values from -4 to 4
- live_blocks: int32 [4, 4, 2], P('gx', 'gy', 'gz'), may hold values from 8 to 32, as said below
Outputs:
- corrected: float32 [3, 64, 64, 512], P(None, 'gx', 'gy', 'gz')
- sweep_history: float32 [2, 5], replicated
The draws below stay inside these ranges and needn't reach their ends.
Inputs may be any that keep to these rules, and one draw needn't show every extreme that they name: `pair_far`: together with far_line: at most one of the three coordinates of node b lies outside the owner block's own nodes; node b lies inside the whole grid; in slots below 16 node b is one of the owner block's own nodes. `far_line`: together with pair_far, as stated there. `live_blocks`: some owner block has all 32 slots live.
All inputs are finite; a program needn't handle non-finite values.
Results may differ from the reference program's by a relative error of at most 0.0001.
Values sent between devices are 32-bit elements; how exact they have to be, the bound alone decides.
A program may use at most 64 MiB of HBM per device.

```python
import jax
import jax.numpy as jnp
from jax import lax

CX = 16
CY = 16
CZ = 256
BLOCKS = 32
PAIRS_BLK = 256
RIM = 3
SWEEPS = 5
NX = 64
NY = 64
NZ = 512
PAIRS_ALL = 262144
N_GX = 4
N_GY = 4
N_GZ = 2


def far_layout(key):
    grid_x = NX // CX
    grid_y = NY // CY
    grid_z = NZ // CZ
    block_shape = (grid_x, grid_y, grid_z, BLOCKS)
    full_shape = (grid_x, grid_y, grid_z, BLOCKS, PAIRS_BLK)
    subkeys = jax.random.split(jax.random.fold_in(key, 7117), 8)
    line_x = jax.random.randint(subkeys[0], block_shape, RIM, CX + RIM)
    line_y = jax.random.randint(subkeys[1], block_shape, RIM, CY + RIM)
    coord_z = jax.random.randint(subkeys[2], full_shape, RIM, CZ + RIM)
    face_axis = jax.random.randint(subkeys[3], block_shape, 0, 3)
    high_block = jax.random.randint(subkeys[4], block_shape, 0, 2)
    layer_block = jax.random.randint(subkeys[5], block_shape, 0, RIM)
    high_pair = jax.random.randint(subkeys[6], full_shape, 0, 2)
    layer_pair = jax.random.randint(subkeys[7], full_shape, 0, RIM)
    rim_slot = lax.broadcasted_iota(jnp.int32, block_shape, 3) >= BLOCKS // 2

    def rim_coord(shape, axis_dim, extent, blocks_along, high_face, rim_layer):
        block_pos = lax.broadcasted_iota(jnp.int32, shape, axis_dim)
        low_side = jnp.where(block_pos == 0, RIM + rim_layer, rim_layer)
        high_side = jnp.where(block_pos == blocks_along - 1, extent + RIM - 1 - rim_layer, extent + RIM + rim_layer)
        return jnp.where(high_face == 1, high_side, low_side)
    line_x = jnp.where(rim_slot & (face_axis == 0), rim_coord(block_shape, 0, CX, grid_x, high_block, layer_block), line_x)
    line_y = jnp.where(rim_slot & (face_axis == 1), rim_coord(block_shape, 1, CY, grid_y, high_block, layer_block), line_y)
    z_face = (rim_slot & (face_axis == 2))[:, :, :, :, None]
    coord_z = jnp.where(z_face, rim_coord(full_shape, 2, CZ, grid_z, high_pair, layer_pair), coord_z)
    return ((line_x * (CY + 2 * RIM) + line_y).astype(jnp.int32), coord_z.astype(jnp.int32))


def draw_pair_far(key, part):
    return far_layout(key)[1]


def draw_far_line(key, part):
    return far_layout(key)[0]


def draw_live_blocks(key, part):
    grid_x = NX // CX
    grid_y = NY // CY
    grid_z = NZ // CZ
    full_shape = (grid_x, grid_y, grid_z)
    subkeys = jax.random.split(key, 3)
    base_count = jax.random.randint(subkeys[0], full_shape, BLOCKS // 4, BLOCKS // 2 + 1)
    heavy_dev = jax.random.randint(subkeys[1], full_shape, 0, 8) == 0
    chosen = jax.random.randint(subkeys[2], (), 0, grid_x * grid_y * grid_z)
    linear = (lax.broadcasted_iota(jnp.int32, full_shape, 0) * grid_y + lax.broadcasted_iota(jnp.int32, full_shape, 1)) * grid_z + lax.broadcasted_iota(jnp.int32, full_shape, 2)
    return jnp.where(heavy_dev | (linear == chosen), BLOCKS, base_count).astype(jnp.int32)


def set_ends(drawn, own_key, low, top_value):
    longest = drawn.shape.index(max(drawn.shape))
    spots = []
    for shift in (0, 1):
        where = [jax.random.randint(jax.random.fold_in(own_key, axis), (), 0, length) for axis, length in enumerate(drawn.shape)]
        where[longest] = (where[longest] + shift) % drawn.shape[longest]
        spots.append(tuple(where))
    return drawn.at[spots[0]].set(low).at[spots[1]].set(top_value)


def shard_levels(stream_key, dims, cuts, least, top_value):
    level = 1.0
    for dim, shards_of in cuts:
        steps = jax.random.uniform(jax.random.fold_in(jax.random.fold_in(stream_key, 6), dim), (shards_of,), jnp.float32, least / len(cuts), top_value / len(cuts))
        level = level * jnp.repeat(jnp.exp(steps), dims[dim] // shards_of).reshape((-1,) + (1,) * (len(dims) - 1 - dim))
    return level


def centred(own_key, shape, width, most, cuts=(), kind=jnp.bfloat16):
    gain = shard_levels(own_key, shape, cuts, -0.22, 0.18) if cuts else 1.0
    drawn = jax.random.normal(own_key, shape, jnp.float32) * width * gain
    return jnp.minimum(jnp.maximum(drawn, -most), most).astype(kind)


def setup_inputs(seed: int = 0) -> dict:
    seeds = jax.random.split(jax.random.key(seed), 8)
    return {
        "positions": centred(seeds[0], (3, NX, NY, NZ), 1.0, 6.0, ((1, 4), (2, 4), (3, 2)), jnp.float32),
        "pair_node": set_ends(jax.random.randint(seeds[1], (N_GX, N_GY, N_GZ, BLOCKS, PAIRS_BLK), 0, CZ), jax.random.fold_in(seeds[1], 1), 0, CZ - 1).astype(jnp.int32),
        "pair_line": set_ends(jax.random.randint(seeds[2], (N_GX, N_GY, N_GZ, BLOCKS), 0, CX * CY), jax.random.fold_in(seeds[2], 1), 0, (CX * CY) - 1).astype(jnp.int32),
        "pair_far": draw_pair_far(jax.random.fold_in(seeds[7], 71), 0),
        "far_line": draw_far_line(jax.random.fold_in(seeds[7], 71), 0),
        "pair_geom": centred(seeds[5], (N_GX, N_GY, N_GZ, BLOCKS, 4, PAIRS_BLK), 0.6, 4.0, ((0, 4), (1, 4), (2, 2)), jnp.float32),
        "live_blocks": draw_live_blocks(jax.random.fold_in(seeds[7], 71), 0),
    }


relax_factor = 0.9

def reference(positions, pair_node, pair_line, pair_far, far_line, pair_geom, live_blocks):
    full_shape = pair_node.shape
    block_x = lax.broadcasted_iota(jnp.int32, full_shape, 0)
    block_y = lax.broadcasted_iota(jnp.int32, full_shape, 1)
    block_z = lax.broadcasted_iota(jnp.int32, full_shape, 2)
    slot_index = lax.broadcasted_iota(jnp.int32, full_shape, 3)
    line_full = jnp.broadcast_to(pair_line[:, :, :, :, None], full_shape)
    node_x = block_x * CX + line_full // CY
    node_y = block_y * CY + line_full % CY
    node_z = block_z * CZ + pair_node
    own_flat = ((node_x * NY + node_y) * NZ + node_z).reshape(-1).astype(jnp.int32)
    ext_y = CY + 2 * RIM
    far_full = jnp.broadcast_to(far_line[:, :, :, :, None], full_shape)
    far_x = far_full // ext_y
    far_y = far_full % ext_y
    far_z = pair_far
    pad_y = NY + 2 * RIM
    pad_z = NZ + 2 * RIM
    far_flat = (((block_x * CX + far_x) * pad_y + block_y * CY + far_y) * pad_z + block_z * CZ + far_z).reshape(-1).astype(jnp.int32)
    live_mask = (slot_index < live_blocks[:, :, :, None, None]).reshape(-1)
    geometry = jnp.moveaxis(pair_geom, 4, 0).reshape(4, -1)
    node_count = NX * NY * NZ
    live_ones = jnp.where(live_mask, 1.0, 0.0).astype(jnp.float32)
    counts = jnp.zeros((node_count,), jnp.float32).at[own_flat].add(live_ones)
    current = positions.reshape(3, -1)
    energies = []
    residuals = []
    for sweep_idx in range(SWEEPS):
        padded = jnp.pad(current.reshape(3, NX, NY, NZ), ((0, 0), (RIM, RIM), (RIM, RIM), (RIM, RIM))).reshape(3, -1)
        differ = current[:, own_flat] - padded[:, far_flat]
        gap_value = lax.optimization_barrier(jnp.sum(geometry[0:3] * differ, axis=0)) - geometry[3]
        depth_value = jnp.where(live_mask, jnp.maximum(-gap_value, 0.0), 0.0)
        energy = jnp.sum(depth_value * depth_value)
        node_total = jnp.zeros((3, node_count), jnp.float32).at[:, own_flat].add(depth_value[None, :] * geometry[0:3])
        scale_factor = 1.0 / (1.0 + energy / PAIRS_ALL)
        correction = relax_factor * scale_factor * node_total / (1.0 + counts)
        current = current + correction
        residuals.append(jnp.sum(correction * correction))
        energies.append(energy)
    history = jnp.stack([jnp.sqrt(1.0 + jnp.stack(energies) / (PAIRS_BLK * BLOCKS)), jnp.sqrt(1.0 + jnp.stack(residuals) / (CX * CY * CZ))])
    return (current.reshape(3, NX, NY, NZ), history)
```

```python
import functools

import jax
import jax.numpy as jnp
from jax import lax
from jax.experimental import pallas as pl
from jax.experimental.pallas import tpu as pltpu
from jax.sharding import PartitionSpec as P

RIM = 3
SWEEPS = 5
RELAX = 0.9
AXES = ("gx", "gy", "gz")
MESH = pl.DeviceIdType.MESH
f32 = jnp.float32
bf16 = jnp.bfloat16


def split(x, parts):
    out = []
    for _ in range(parts - 1):
        hi = x.astype(bf16)
        out.append(hi)
        x = x - hi.astype(f32)
    out.append(x.astype(bf16))
    return out


def mm(a, b):
    return jnp.dot(a, b, preferred_element_type=f32)


def take_lanes(x, low, half):
    outs = []
    for h in range(0, low.shape[1], 128):
        idx = low[:, h : h + 128]
        got = jnp.take_along_axis(x[:, :128], idx, axis=1, mode="promise_in_bounds")
        for j in range(1, x.shape[1] // 128):
            more = jnp.take_along_axis(
                x[:, 128 * j : 128 * (j + 1)], idx, axis=1, mode="promise_in_bounds"
            )
            got = jnp.where(half[:, h : h + 128] == j, more, got)
        outs.append(got)
    return jnp.concatenate(outs, axis=1)


def kernel(
    sizes,
    blk,
    live_ref,
    pk_ref,
    pos_ref,
    out_ref,
    hist_ref,
    hot,
    two,
    amat,
    cinv,
    geo,
    low_ref,
    half_ref,
    gap,
    acc,
    wcat,
    reqs,
    dsend,
    drecv,
    erecv,
    rrecv,
    evals,
    qs_sem,
    qr_sem,
    ds_sem,
    dr_sem,
    es_sem,
    er_sem,
    rs_sem,
    rr_sem,
):
    nx, ny, nz = sizes
    bx, by, bz = blk
    devices = nx * ny * nz
    blocks = pk_ref.shape[1]
    pairs = pk_ref.shape[2]
    outer = blocks // 2
    lines = bx * by
    me = [lax.axis_index(a) for a in AXES]
    mine = (me[0] * ny + me[1]) * nz + me[2]
    dirs = [(a, s) for a in range(3) for s in (1, -1)]

    def neighbour(axis, sign):
        to = list(me)
        to[axis] = lax.rem(me[axis] + sign + sizes[axis], sizes[axis])
        return tuple(to)

    def coords(k):
        to = lax.rem(mine + k, devices)
        return (to // (ny * nz), lax.rem(to // nz, ny), lax.rem(to, nz))

    for d, (axis, sign) in enumerate(dirs):
        pltpu.make_async_remote_copy(
            src_ref=pk_ref.at[pl.ds(0, 5), pl.ds(outer, outer)],
            dst_ref=reqs.at[d],
            send_sem=qs_sem,
            recv_sem=qr_sem,
            device_id=neighbour(axis, sign),
            device_id_type=MESH,
        ).start()

    live = live_ref[0]
    live_rows = lax.broadcasted_iota(jnp.int32, (blocks, pairs), 0) < live
    lane_node = lax.broadcasted_iota(jnp.int32, (pairs, bz), 1).astype(f32)
    node_t = jnp.transpose(pk_ref[6])
    for b in range(blocks):
        hot[pl.ds(b * pairs, pairs), :] = jnp.where(
            node_t[:, b : b + 1] == lane_node, 1.0, 0.0
        ).astype(bf16)
    line_b = pk_ref[7]
    two[...] = jnp.transpose(jnp.concatenate([line_b, line_b], axis=0))
    row_mod = lax.broadcasted_iota(jnp.int32, (blocks, 2 * blocks), 0)
    col_mod = lax.rem(lax.broadcasted_iota(jnp.int32, (blocks, 2 * blocks), 1), blocks)
    same = line_b[:, : 2 * blocks] == two[0:blocks, :]
    first_row = 1.0 - jnp.max(
        jnp.where(same & (row_mod < col_mod), 1.0, 0.0), axis=0, keepdims=True
    )
    first_col = 1.0 - jnp.max(
        jnp.where(same & (col_mod < row_mod), 1.0, 0.0), axis=1, keepdims=True
    )
    line_rows = lax.broadcasted_iota(jnp.int32, (lines, 2 * blocks), 0).astype(f32)
    lane_line = lax.broadcasted_iota(jnp.int32, (blocks, lines), 1).astype(f32)

    def expand(stack, step):
        rows = stack.shape[0]
        which = lax.rem(lax.broadcasted_iota(jnp.int32, (rows, pairs), 0), step)
        return jnp.concatenate(
            [jnp.where(which == j, stack, 0.0).astype(bf16) for j in range(step)], axis=1
        )

    counts = []
    for g in range(blocks // 8):
        ones = jnp.where(live_rows[8 * g : 8 * g + 8], 1.0, 0.0)
        counts.append(mm(expand(ones, 8), hot[pl.ds(8 * g * pairs, 8 * pairs), :]))
    counts = jnp.concatenate(counts, axis=0).astype(bf16)

    pos_parts = [split(pos_ref[c].reshape(lines, bz), 3) for c in range(3)]

    def setup(row, n, line, node, valid, geom, sign):
        sel = line[:, : 2 * blocks] == two[0:n, :]
        a = jnp.where(sel, 1.0, 0.0)
        amat[pl.ds(row, n), :] = a.astype(bf16)
        cnt = mm(a[:, :blocks].astype(bf16), counts)
        cinv[pl.ds(row, n), :] = RELAX / (1.0 + cnt)
        idx = jnp.where(valid, node, 0.0).astype(jnp.int32)
        low_ref[pl.ds(row, n), :] = lax.rem(idx, 128)
        half_ref[pl.ds(row, n), :] = idx // 128
        own = jnp.where(line == lane_line[:n], 1.0, 0.0).astype(bf16)
        total = jnp.zeros((n, pairs), f32)
        for c in range(3):
            gc = jnp.where(valid, geom[c], 0.0) * sign
            geo[c, pl.ds(row, n), :] = gc
            vals = mm(own, pos_parts[c][0]) + mm(own, pos_parts[c][1]) + mm(own, pos_parts[c][2])
            total += gc * take_lanes(vals, low_ref[pl.ds(row, n), :], half_ref[pl.ds(row, n), :])
        return total

    def located(code, zpos, shift):
        e = jnp.floor((code + 0.5) / (by + 2 * RIM))
        f = code - e * (by + 2 * RIM)
        e = e - (RIM + shift[0] * bx)
        f = f - (RIM + shift[1] * by)
        z = zpos - (RIM + shift[2] * bz)
        ok_line = (e >= 0) & (e < bx) & (f >= 0) & (f < by)
        return jnp.where(ok_line, e * by + f, -1.0), z, ok_line & (z >= 0) & (z < bz)

    geom_own = [pk_ref[c] for c in range(3)]
    start = setup(0, blocks, line_b, pk_ref[6], line_b >= 0, geom_own, 1.0)
    line, z, ok = located(pk_ref[4], pk_ref[3], (0, 0, 0))
    start += setup(blocks, blocks, line, z, ok, geom_own, -1.0)
    gap[...] = start - pk_ref[5]
    acc[...] = jnp.zeros_like(acc)

    pltpu.make_async_copy(reqs, reqs, qr_sem).wait()
    base = 2 * blocks
    for d, (axis, sign) in enumerate(dirs):
        shift = [0, 0, 0]
        shift[axis] = sign
        line, z, ok = located(reqs[d, 4], reqs[d, 3], shift)
        geom = [reqs[d, c] for c in range(3)]
        dsend[0, d] = setup(base + d * outer, outer, line, z, ok, geom, -1.0)

    def respond(t):
        for d, (axis, sign) in enumerate(dirs):
            pltpu.make_async_remote_copy(
                src_ref=dsend.at[t, d],
                dst_ref=drecv.at[t, d],
                send_sem=ds_sem.at[t],
                recv_sem=dr_sem.at[t],
                device_id=neighbour(axis, -sign),
                device_id_type=MESH,
            ).start()

    def received(t):
        pltpu.make_async_copy(drecv.at[t], drecv.at[t], dr_sem.at[t]).wait()
        got = drecv[t, 0]
        for d in range(1, len(dirs)):
            got = got + drecv[t, d]
        return got

    respond(0)
    gap[pl.ds(outer, outer), :] = gap[pl.ds(outer, outer), :] + received(0)

    def to_all(ref, send_sem, recv_sem):
        def send(k, carry):
            pltpu.make_async_remote_copy(
                src_ref=ref,
                dst_ref=ref,
                send_sem=send_sem,
                recv_sem=recv_sem,
                device_id=coords(k),
                device_id_type=MESH,
            ).start()
            return carry

        lax.fori_loop(1, devices, send, 0)

    def lanes_sum(x):
        x = jnp.sum(x, axis=0, keepdims=True)
        out = x[:, :128]
        for j in range(1, x.shape[1] // 128):
            out = out + x[:, 128 * j : 128 * (j + 1)]
        return out

    def sweep(t, last):
        depth = jnp.where(live_rows, jnp.maximum(-gap[...], 0.0), 0.0)
        erecv[t, mine] = lanes_sum(depth * depth)
        to_all(erecv.at[t, mine], es_sem.at[t], er_sem.at[t])
        for g in range(blocks // 8):
            lo, hi = 8 * g, 8 * g + 8
            terms = jnp.concatenate([depth[lo:hi] * pk_ref[c, lo:hi] for c in range(3)], axis=0)
            top = terms.astype(bf16).astype(f32)
            stack = jnp.concatenate([top, terms - top], axis=0)
            sums = mm(expand(stack, 8), hot[pl.ds(lo * pairs, 8 * pairs), :])
            sums = sums[:24] + sums[24:]
            for c in range(3):
                wcat[lo:hi, c * bz : (c + 1) * bz] = sums[8 * c : 8 * c + 8]
        parts = jnp.concatenate(split(wcat[...], 2), axis=0)
        rows = blocks if last else amat.shape[0]
        both = mm(amat[0:rows, :], parts)
        moved = [both[:, c * bz : (c + 1) * bz] * cinv[0:rows, :] for c in range(3)]
        near = jnp.concatenate([m[:blocks] for m in moved], axis=1)
        rrecv[mine, pl.ds(t, 1), :] = lanes_sum(near * near * first_col)
        if last:
            to_all(rrecv.at[mine], rs_sem, rr_sem)
        else:
            total = geo[0] * take_lanes(moved[0], low_ref[...], half_ref[...])
            for c in range(1, 3):
                total += geo[c] * take_lanes(moved[c], low_ref[...], half_ref[...])
            for d in range(len(dirs)):
                dsend[t + 1, d] = total[base + d * outer : base + (d + 1) * outer]
            respond(t + 1)
            step = total[:blocks] + total[blocks : 2 * blocks]
        others = erecv.at[t, pl.ds(0, devices - 1)]
        pltpu.make_async_copy(others, others, er_sem.at[t]).wait()
        energy = jnp.sum(jnp.sum(erecv[t], axis=0), axis=1, keepdims=True)
        scale = 1.0 / (1.0 + energy / (blocks * pairs * devices))
        evals[0, pl.ds(t, 1), :] = jnp.broadcast_to(energy, (1, 128))
        evals[1, pl.ds(t, 1), :] = jnp.broadcast_to(scale, (1, 128))
        acc[...] = acc[...] + scale * near
        if not last:
            more = received(t + 1)
            gap[0:outer, :] = gap[0:outer, :] + scale * step[:outer]
            gap[pl.ds(outer, outer), :] = gap[pl.ds(outer, outer), :] + scale * (
                step[outer:] + more
            )

    rrecv[mine] = jnp.zeros(rrecv.shape[1:], f32)
    evals[...] = jnp.zeros_like(evals)

    def body(t, carry):
        sweep(t, False)
        return carry

    lax.fori_loop(0, SWEEPS - 1, body, 0)
    sweep(SWEEPS - 1, True)

    place = jnp.where(line_rows == two[...], 1.0, 0.0) * first_row
    place = place.astype(bf16)
    total = mm(place, jnp.concatenate(split(acc[...], 2), axis=0))
    for c in range(3):
        out_ref[c] = pos_ref[c] + total[:, c * bz : (c + 1) * bz].reshape(bx, by, bz)

    others = rrecv.at[pl.ds(0, devices - 1)]
    pltpu.make_async_copy(others, others, rr_sem).wait()
    resid = jnp.sum(jnp.sum(rrecv[...], axis=0), axis=1, keepdims=True)
    scales = evals[1]
    hist_ref[0] = jnp.sqrt(1.0 + evals[0] / (blocks * pairs))
    hist_ref[1] = jnp.sqrt(1.0 + scales * scales * resid / (bx * by * bz))

    pltpu.make_async_copy(reqs, reqs, qs_sem).wait()
    for t in range(SWEEPS):
        pltpu.make_async_copy(dsend.at[t], dsend.at[t], ds_sem.at[t]).wait()
        ref = erecv.at[t, pl.ds(0, devices - 1)]
        pltpu.make_async_copy(ref, ref, es_sem.at[t]).wait()
    pltpu.make_async_copy(others, others, rs_sem).wait()


def local(sizes, positions, pair_node, pair_line, pair_far, far_line, pair_geom, live_blocks):
    within = pair_node[0, 0, 0]
    blocks, pairs = within.shape
    blk = positions.shape[1:]
    geometry = jnp.moveaxis(pair_geom[0, 0, 0], 1, 0)

    def wide(x):
        return jnp.broadcast_to(x[:, None], (blocks, pairs)).astype(f32)

    packed = jnp.stack(
        [
            geometry[0],
            geometry[1],
            geometry[2],
            pair_far[0, 0, 0].astype(f32),
            wide(far_line[0, 0, 0]),
            geometry[3],
            within.astype(f32),
            wide(pair_line[0, 0, 0]),
        ]
    )
    devices = sizes[0] * sizes[1] * sizes[2]
    outer = blocks // 2
    rows = 2 * blocks + 6 * outer
    dma = pltpu.SemaphoreType.DMA
    vmem = pl.BlockSpec(memory_space=pltpu.VMEM)
    corrected, hist = pl.pallas_call(
        functools.partial(kernel, sizes, blk),
        out_shape=(
            jax.ShapeDtypeStruct(positions.shape, f32),
            jax.ShapeDtypeStruct((2, 8, 128), f32),
        ),
        in_specs=[pl.BlockSpec(memory_space=pltpu.SMEM), vmem, vmem],
        out_specs=(vmem, vmem),
        scratch_shapes=[
            pltpu.VMEM((blocks * pairs, blk[2]), bf16),
            pltpu.VMEM((pairs, 2 * blocks), f32),
            pltpu.VMEM((rows, 2 * blocks), bf16),
            pltpu.VMEM((rows, pairs), f32),
            pltpu.VMEM((3, rows, pairs), f32),
            pltpu.VMEM((rows, pairs), jnp.int32),
            pltpu.VMEM((rows, pairs), jnp.int32),
            pltpu.VMEM((blocks, pairs), f32),
            pltpu.VMEM((blocks, 3 * blk[2]), f32),
            pltpu.VMEM((blocks, 3 * blk[2]), f32),
            pltpu.VMEM((6, 5, outer, pairs), f32),
            pltpu.VMEM((SWEEPS, 6, outer, pairs), f32),
            pltpu.VMEM((SWEEPS, 6, outer, pairs), f32),
            pltpu.VMEM((SWEEPS, devices, 1, 128), f32),
            pltpu.VMEM((devices, 8, 128), f32),
            pltpu.VMEM((2, 8, 128), f32),
            dma,
            dma,
            dma((SWEEPS,)),
            dma((SWEEPS,)),
            dma((SWEEPS,)),
            dma((SWEEPS,)),
            dma,
            dma,
        ],
        compiler_params=pltpu.CompilerParams(has_side_effects=True),
    )(live_blocks.reshape(1), packed, positions)
    return corrected, hist[:, :SWEEPS, 0]


def solution(mesh):
    sizes = tuple(mesh.shape[a] for a in AXES)
    return jax.shard_map(
        functools.partial(local, sizes),
        mesh=mesh,
        in_specs=(
            P(None, "gx", "gy", "gz"),
            P("gx", "gy", "gz", None, None),
            P("gx", "gy", "gz", None),
            P("gx", "gy", "gz", None, None),
            P("gx", "gy", "gz", None),
            P("gx", "gy", "gz", None, None, None),
            P("gx", "gy", "gz"),
        ),
        out_specs=(P(None, "gx", "gy", "gz"), P()),
        check_vma=False,
    )
```

```python
import functools

import jax
import jax.numpy as jnp
from jax import lax
from jax.experimental import pallas as pl
from jax.experimental.pallas import tpu as pltpu
from jax.sharding import PartitionSpec as P

RIM = 3
SWEEPS = 5
RELAX = 0.9
AXES = ("gx", "gy", "gz")
MESH = pl.DeviceIdType.MESH
f32 = jnp.float32
bf16 = jnp.bfloat16


def split(x, parts):
    out = []
    for _ in range(parts - 1):
        hi = x.astype(bf16)
        out.append(hi)
        x = x - hi.astype(f32)
    out.append(x.astype(bf16))
    return out


def mm(a, b):
    return jnp.dot(a, b, preferred_element_type=f32)


def take_lanes(x, low, half):
    outs = []
    for h in range(0, low.shape[1], 128):
        idx = low[:, h : h + 128]
        got = jnp.take_along_axis(x[:, :128], idx, axis=1, mode="promise_in_bounds")
        for j in range(1, x.shape[1] // 128):
            more = jnp.take_along_axis(
                x[:, 128 * j : 128 * (j + 1)], idx, axis=1, mode="promise_in_bounds"
            )
            got = jnp.where(half[:, h : h + 128] == j, more, got)
        outs.append(got)
    return jnp.concatenate(outs, axis=1)


def kernel(
    sizes,
    blk,
    live_ref,
    node_ref,
    line_ref,
    farpos_ref,
    farline_ref,
    geom_ref,
    pos_hbm,
    acc_ref,
    hist_ref,
    pos_ref,
    req,
    cols,
    hot,
    two,
    amat,
    cinv,
    geo,
    low_ref,
    half_ref,
    gap,
    wcat,
    reqs,
    dsend,
    drecv,
    erecv,
    rrecv,
    pos_sem,
    qs_sem,
    qr_sem,
    ds_sem,
    dr_sem,
    es_sem,
    er_sem,
    rs_sem,
    rr_sem,
):
    nx, ny, nz = sizes
    bx, by, bz = blk
    devices = nx * ny * nz
    blocks, pairs = gap.shape
    outer = blocks // 2
    lines = bx * by
    me = [lax.axis_index(a) for a in AXES]
    mine = (me[0] * ny + me[1]) * nz + me[2]
    dirs = [(a, s) for a in range(3) for s in (1, -1)]

    def neighbour(axis, sign):
        to = list(me)
        to[axis] = lax.rem(me[axis] + sign + sizes[axis], sizes[axis])
        return tuple(to)

    def coords(k):
        to = lax.rem(mine + k, devices)
        return (to // (ny * nz), lax.rem(to // nz, ny), lax.rem(to, nz))

    pos_copy = pltpu.make_async_copy(pos_hbm, pos_ref, pos_sem)
    pos_copy.start()

    def column(ref):
        row = ref[0, 0].astype(f32)
        return jnp.transpose(jnp.broadcast_to(row, (pairs, blocks)))

    for c in range(3):
        req[c] = geom_ref[0, 0, 0, outer:, c, :]
    req[3] = farpos_ref[0, 0, 0, outer:, :].astype(f32)
    cols[1] = column(farline_ref)
    req[4] = cols[1, outer:, :]
    cols[0] = column(line_ref)
    for d, (axis, sign) in enumerate(dirs):
        pltpu.make_async_remote_copy(
            src_ref=req,
            dst_ref=reqs.at[d],
            send_sem=qs_sem,
            recv_sem=qr_sem,
            device_id=neighbour(axis, sign),
            device_id_type=MESH,
        ).start()

    live = jnp.broadcast_to(live_ref[0], (blocks, pairs))
    live_rows = lax.broadcasted_iota(jnp.int32, (blocks, pairs), 0) < live
    lane_node = lax.broadcasted_iota(jnp.int32, (pairs, bz), 1).astype(f32)
    node_t = jnp.transpose(node_ref[0, 0, 0].astype(f32))
    for b in range(blocks):
        hot[pl.ds(b * pairs, pairs), :] = jnp.where(
            node_t[:, b : b + 1] == lane_node, 1.0, 0.0
        ).astype(bf16)
    row_line = line_ref[0, 0].astype(f32)
    two[...] = jnp.concatenate([row_line, row_line], axis=1)
    row_mod = lax.broadcasted_iota(jnp.int32, (blocks, blocks), 0)
    col_mod = lax.broadcasted_iota(jnp.int32, (blocks, blocks), 1)
    line_b = cols[0]
    same = line_b[:, :blocks] == row_line
    first_col = 1.0 - jnp.max(
        jnp.where(same & (col_mod < row_mod), 1.0, 0.0), axis=1, keepdims=True
    )

    def expand(stack, step):
        rows = stack.shape[0]
        which = lax.rem(lax.broadcasted_iota(jnp.int32, (rows, pairs), 0), step)
        return jnp.concatenate(
            [jnp.where(which == j, stack, 0.0).astype(bf16) for j in range(step)], axis=1
        )

    counts = []
    for g in range(blocks // 8):
        ones = jnp.where(live_rows[8 * g : 8 * g + 8], 1.0, 0.0)
        counts.append(mm(expand(ones, 8), hot[pl.ds(8 * g * pairs, 8 * pairs), :]))
    counts = jnp.concatenate(counts, axis=0).astype(bf16)

    def located(code, zpos, shift):
        e = jnp.floor((code + 0.5) / (by + 2 * RIM))
        f = code - e * (by + 2 * RIM)
        e = e - (RIM + shift[0] * bx)
        f = f - (RIM + shift[1] * by)
        z = zpos - (RIM + shift[2] * bz)
        ok_line = (e >= 0) & (e < bx) & (f >= 0) & (f < by)
        return jnp.where(ok_line, e * by + f, -1.0), z, ok_line & (z >= 0) & (z < bz)

    def setup(row, line, node, geom):
        n = line.shape[0]
        lane_line = lax.broadcasted_iota(jnp.int32, (n, lines), 1).astype(f32)
        a = jnp.where(line[:, : 2 * blocks] == two[...], 1.0, 0.0).astype(bf16)
        amat[pl.ds(row, n), :] = a
        cinv[pl.ds(row, n), :] = RELAX / (1.0 + mm(a[:, :blocks], counts))
        idx = node.astype(jnp.int32)
        low = lax.bitwise_and(idx, 127)
        half = lax.shift_right_logical(idx, 7)
        low_ref[pl.ds(row, n), :] = low
        half_ref[pl.ds(row, n), :] = half
        own = jnp.where(line == lane_line, 1.0, 0.0).astype(bf16)
        total = jnp.zeros((n, pairs), f32)
        for c in range(3):
            geo[c, pl.ds(row, n), :] = geom[c]
            vals = jnp.zeros((n, bz), f32)
            for part in split(pos_ref[c].reshape(lines, bz), 3):
                vals += mm(own, part)
            total += geom[c] * take_lanes(vals, low, half)
        return total

    def cat(parts):
        return jnp.concatenate(parts, axis=0)

    pos_copy.wait()
    pltpu.make_async_copy(reqs, reqs, qr_sem).wait()
    asked = []
    for d, (axis, sign) in enumerate(dirs):
        shift = [0, 0, 0]
        shift[axis] = sign
        line, z, ok = located(reqs[d, 4], reqs[d, 3], shift)
        asked.append(
            [line, jnp.where(ok, z, 0.0)] + [jnp.where(ok, -reqs[d, c], 0.0) for c in range(3)]
        )
    asked = [cat([x[i] for x in asked]) for i in range(5)]
    base = asked[0].shape[0]
    rows = base + 2 * blocks

    def respond(t, total):
        for d, (axis, sign) in enumerate(dirs):
            dsend[t, d] = total[d * outer : (d + 1) * outer]
        for d, (axis, sign) in enumerate(dirs):
            pltpu.make_async_remote_copy(
                src_ref=dsend.at[t, d],
                dst_ref=drecv.at[t, d],
                send_sem=ds_sem.at[t],
                recv_sem=dr_sem.at[t],
                device_id=neighbour(axis, -sign),
                device_id_type=MESH,
            ).start()

    def received(t):
        pltpu.make_async_copy(drecv.at[t], drecv.at[t], dr_sem.at[t]).wait()
        got = drecv[t, 0]
        for d in range(1, len(dirs)):
            got = got + drecv[t, d]
        return got

    respond(0, setup(0, asked[0], asked[1], asked[2:]))

    line, z, ok = located(cols[1], farpos_ref[0, 0, 0].astype(f32), (0, 0, 0))
    geom = [geom_ref[0, 0, 0, :, c, :] for c in range(4)]
    start = setup(
        base,
        cat([line_b, line]),
        cat([node_ref[0, 0, 0].astype(f32), jnp.where(ok, z, 0.0)]),
        [cat([geom[c], jnp.where(ok, -geom[c], 0.0)]) for c in range(3)],
    )
    start = start[:blocks] + start[blocks:] - geom[3]
    gap[0:outer, :] = start[:outer]
    gap[pl.ds(outer, outer), :] = start[outer:] + received(0)
    acc_ref[...] = jnp.zeros_like(acc_ref)

    def to_all(ref, send_sem, recv_sem):
        def send(k, carry):
            pltpu.make_async_remote_copy(
                src_ref=ref,
                dst_ref=ref,
                send_sem=send_sem,
                recv_sem=recv_sem,
                device_id=coords(k),
                device_id_type=MESH,
            ).start()
            return carry

        lax.fori_loop(1, devices, send, 0)

    def lanes_sum(x):
        x = jnp.sum(x, axis=0, keepdims=True)
        out = x[:, :128]
        for j in range(1, x.shape[1] // 128):
            out = out + x[:, 128 * j : 128 * (j + 1)]
        return out

    lane = lax.broadcasted_iota(jnp.int32, (1, 128), 1)

    def apply(row, n, parts):
        both = mm(amat[row : row + n, :], parts)
        return [both[:, c * bz : (c + 1) * bz] * cinv[row : row + n, :] for c in range(3)]

    def dots(row, n, moved):
        low = low_ref[row : row + n, :]
        half = half_ref[row : row + n, :]
        total = geo[0, row : row + n] * take_lanes(moved[0], low, half)
        for c in range(1, 3):
            total += geo[c, row : row + n] * take_lanes(moved[c], low, half)
        return total

    def sweep(t, last):
        depth = jnp.where(live_rows, jnp.maximum(-gap[...], 0.0), 0.0)
        erecv[t, mine] = lanes_sum(depth * depth)
        to_all(erecv.at[t, mine], es_sem.at[t], er_sem.at[t])
        for g in range(blocks // 8):
            lo, hi = 8 * g, 8 * g + 8
            terms = cat([depth[lo:hi] * geo[c, base + lo : base + hi] for c in range(3)])
            top = terms.astype(bf16).astype(f32)
            sums = mm(expand(cat([top, terms - top]), 8), hot[pl.ds(lo * pairs, 8 * pairs), :])
            sums = sums[:24] + sums[24:]
            for c in range(3):
                wcat[lo:hi, c * bz : (c + 1) * bz] = sums[8 * c : 8 * c + 8]
        parts = cat(split(wcat[...], 2))
        if not last:
            respond(t + 1, dots(0, base, apply(0, base, parts)))
        moved = apply(base, blocks if last else 2 * blocks, parts)
        near = jnp.concatenate([m[:blocks] for m in moved], axis=1)
        resid = jnp.sum(lanes_sum(near * near * first_col), axis=1, keepdims=True)
        rrecv[mine] = jnp.where(lane == t, resid, rrecv[mine])
        if last:
            to_all(rrecv.at[mine], rs_sem, rr_sem)
        else:
            step = dots(base, 2 * blocks, moved)
            step = step[:blocks] + step[blocks:]
        others = erecv.at[t, pl.ds(0, devices - 1)]
        pltpu.make_async_copy(others, others, er_sem.at[t]).wait()
        energy = jnp.sum(jnp.sum(erecv[t], axis=0), axis=1, keepdims=True)
        scale = 1.0 / (1.0 + energy / (blocks * pairs * devices))
        hist_ref[0:1, :] = jnp.where(lane == t, energy, hist_ref[0:1, :])
        hist_ref[1:2, :] = jnp.where(lane == t, scale, hist_ref[1:2, :])
        acc_ref[...] = acc_ref[...] + (scale * first_col) * near
        if not last:
            more = received(t + 1)
            gap[0:outer, :] = gap[0:outer, :] + scale * step[:outer]
            gap[pl.ds(outer, outer), :] = gap[pl.ds(outer, outer), :] + scale * (
                step[outer:] + more
            )

    rrecv[mine] = jnp.zeros((1, 128), f32)
    hist_ref[...] = jnp.zeros_like(hist_ref)

    def body(t, carry):
        sweep(t, False)
        return carry

    lax.fori_loop(0, SWEEPS - 1, body, 0)
    sweep(SWEEPS - 1, True)

    pltpu.make_async_copy(reqs, reqs, qs_sem).wait()
    for t in range(SWEEPS):
        pltpu.make_async_copy(dsend.at[t], dsend.at[t], ds_sem.at[t]).wait()
        ref = erecv.at[t, pl.ds(0, devices - 1)]
        pltpu.make_async_copy(ref, ref, es_sem.at[t]).wait()
    others = rrecv.at[pl.ds(0, devices - 1)]
    pltpu.make_async_copy(others, others, rs_sem).wait()
    pltpu.make_async_copy(others, others, rr_sem).wait()
    energy, scale = hist_ref[0:1, :], hist_ref[1:2, :]
    resid = jnp.sum(rrecv[...], axis=0)
    hist_ref[0:1, :] = jnp.sqrt(1.0 + energy / (blocks * pairs))
    hist_ref[1:2, :] = jnp.sqrt(1.0 + scale * scale * resid / (bx * by * bz))


def finish(acc_ref, line_ref, hist_in, pos_ref, out_ref, hist_ref):
    _, bx, by, bz = pos_ref.shape
    lines = bx * by
    row = line_ref[0, 0].astype(f32)
    row = jnp.concatenate([row, row], axis=1)
    rows = lax.broadcasted_iota(jnp.int32, (lines, row.shape[1]), 0).astype(f32)
    place = jnp.where(rows == row, 1.0, 0.0).astype(bf16)
    total = mm(place, jnp.concatenate(split(acc_ref[...], 2), axis=0))
    out_ref[0] = pos_ref[0] + total.reshape(bx, by, bz)
    hist_ref[...] = hist_in[0:2, : hist_ref.shape[1]]


def local(sizes, positions, pair_node, pair_line, pair_far, far_line, pair_geom, live_blocks):
    blocks, pairs = pair_node.shape[3:]
    blk = positions.shape[1:]
    devices = sizes[0] * sizes[1] * sizes[2]
    outer = blocks // 2
    rows = 2 * blocks + 6 * outer
    dma = pltpu.SemaphoreType.DMA
    vmem = pl.BlockSpec(memory_space=pltpu.VMEM)
    moved, hist = pl.pallas_call(
        functools.partial(kernel, sizes, blk),
        out_shape=(
            jax.ShapeDtypeStruct((blocks, 3 * blk[2]), f32),
            jax.ShapeDtypeStruct((8, 128), f32),
        ),
        in_specs=[vmem] * 6

        + [pl.BlockSpec(memory_space=pl.ANY)],
        out_specs=(vmem, vmem),
        scratch_shapes=[
            pltpu.VMEM(positions.shape, f32),
            pltpu.VMEM((5, outer, pairs), f32),
            pltpu.VMEM((2, blocks, pairs), f32),
            pltpu.VMEM((blocks * pairs, blk[2]), bf16),
            pltpu.VMEM((1, 2 * blocks), f32),
            pltpu.VMEM((rows, 2 * blocks), bf16),
            pltpu.VMEM((rows, pairs), f32),
            pltpu.VMEM((3, rows, pairs), f32),
            pltpu.VMEM((rows, pairs), jnp.int32),
            pltpu.VMEM((rows, pairs), jnp.int32),
            pltpu.VMEM((blocks, pairs), f32),
            pltpu.VMEM((blocks, 3 * blk[2]), f32),
            pltpu.VMEM((6, 5, outer, pairs), f32),
            pltpu.VMEM((SWEEPS, 6, outer, pairs), f32),
            pltpu.VMEM((SWEEPS, 6, outer, pairs), f32),
            pltpu.VMEM((SWEEPS, devices, 1, 128), f32),
            pltpu.VMEM((devices, 1, 128), f32),
            dma,
            dma,
            dma,
            dma((SWEEPS,)),
            dma((SWEEPS,)),
            dma((SWEEPS,)),
            dma((SWEEPS,)),
            dma,
            dma,
        ],
        compiler_params=pltpu.CompilerParams(has_side_effects=True),
    )(live_blocks, pair_node, pair_line, pair_far, far_line, pair_geom, positions)
    return pl.pallas_call(
        finish,
        grid=(3,),
        out_shape=(
            jax.ShapeDtypeStruct(positions.shape, f32),
            jax.ShapeDtypeStruct((2, SWEEPS), f32),
        ),
        in_specs=[
            pl.BlockSpec((blocks, blk[2]), lambda c: (0, c)),
            pl.BlockSpec(pair_line.shape, lambda c: (0, 0, 0, 0)),
            pl.BlockSpec((8, 128), lambda c: (0, 0)),
            pl.BlockSpec((1,) + blk, lambda c: (c, 0, 0, 0)),
        ],
        out_specs=(
            pl.BlockSpec((1,) + blk, lambda c: (c, 0, 0, 0)),
            pl.BlockSpec((2, SWEEPS), lambda c: (0, 0)),
        ),
    )(moved, pair_line, hist, positions)


def solution(mesh):
    sizes = tuple(mesh.shape[a] for a in AXES)
    return jax.shard_map(
        functools.partial(local, sizes),
        mesh=mesh,
        in_specs=(
            P(None, "gx", "gy", "gz"),
            P("gx", "gy", "gz", None, None),
            P("gx", "gy", "gz", None),
            P("gx", "gy", "gz", None, None),
            P("gx", "gy", "gz", None),
            P("gx", "gy", "gz", None, None, None),
            P("gx", "gy", "gz"),
        ),
        out_specs=(P(None, "gx", "gy", "gz"), P()),
        check_vma=False,
    )
```

```python
import functools

import jax
import jax.numpy as jnp
from jax import lax
from jax.experimental import pallas as pl
from jax.experimental.pallas import tpu as pltpu
from jax.sharding import PartitionSpec as P

RIM = 3
SWEEPS = 5
RELAX = 0.9
AXES = ("gx", "gy", "gz")
MESH = pl.DeviceIdType.MESH
f32 = jnp.float32
bf16 = jnp.bfloat16


def split(x, parts):
    out = []
    for _ in range(parts - 1):
        hi = x.astype(bf16)
        out.append(hi)
        x = x - hi.astype(f32)
    out.append(x.astype(bf16))
    return out


def mm(a, b):
    return jnp.dot(a, b, preferred_element_type=f32)


def take_lanes(x, low, half):
    outs = []
    for h in range(0, low.shape[1], 128):
        idx = low[:, h : h + 128]
        got = jnp.take_along_axis(x[:, :128], idx, axis=1, mode="promise_in_bounds")
        for j in range(1, x.shape[1] // 128):
            more = jnp.take_along_axis(
                x[:, 128 * j : 128 * (j + 1)], idx, axis=1, mode="promise_in_bounds"
            )
            got = jnp.where(half[:, h : h + 128] == j, more, got)
        outs.append(got)
    return jnp.concatenate(outs, axis=1)


def kernel(
    sizes,
    blk,
    live_ref,
    node_ref,
    line_ref,
    farpos_ref,
    farline_ref,
    geom_ref,
    pos_hbm,
    acc_ref,
    hist_ref,
    pos_ref,
    req,
    cols,
    hot,
    two,
    amat,
    cinv,
    geo,
    low_ref,
    half_ref,
    gap,
    wcat,
    reqs,
    dsend,
    drecv,
    erecv,
    rrecv,
    pos_sem,
    qs_sem,
    qr_sem,
    ds_sem,
    dr_sem,
    es_sem,
    er_sem,
    rs_sem,
    rr_sem,
):
    nx, ny, nz = sizes
    bx, by, bz = blk
    devices = nx * ny * nz
    blocks, pairs = gap.shape
    outer = blocks // 2
    lines = bx * by
    me = [lax.axis_index(a) for a in AXES]
    mine = (me[0] * ny + me[1]) * nz + me[2]
    dirs = [(a, s) for a in (1, 0, 2) for s in (1, -1)]

    def neighbour(axis, sign):
        to = list(me)
        to[axis] = lax.rem(me[axis] + sign + sizes[axis], sizes[axis])
        return tuple(to)

    def exists(axis, sign):
        return (me[axis] + sign >= 0) & (me[axis] + sign < sizes[axis])

    def coords(k):
        to = lax.rem(mine + k, devices)
        return (to // (ny * nz), lax.rem(to // nz, ny), lax.rem(to, nz))

    pos_copy = pltpu.make_async_copy(pos_hbm, pos_ref, pos_sem)
    pos_copy.start()

    def column(ref):
        row = ref[0, 0].astype(f32)
        return jnp.transpose(jnp.broadcast_to(row, (pairs, blocks)))

    for c in range(3):
        req[c] = geom_ref[0, 0, 0, outer:, c, :]
    req[3] = farpos_ref[0, 0, 0, outer:, :].astype(f32)
    cols[1] = column(farline_ref)
    req[4] = cols[1, outer:, :]
    cols[0] = column(line_ref)
    def ask(d, axis, sign):
        return pltpu.make_async_remote_copy(
            src_ref=req,
            dst_ref=reqs.at[d],
            send_sem=qs_sem.at[d],
            recv_sem=qr_sem.at[d],
            device_id=neighbour(axis, sign),
            device_id_type=MESH,
        )

    for d, (axis, sign) in enumerate(dirs):

        @pl.when(exists(axis, sign))
        def _():
            ask(d, axis, sign).start()

    for d, (axis, sign) in enumerate(dirs):

        @pl.when(jnp.logical_not(exists(axis, -sign)))
        def _():
            reqs[d] = jnp.zeros(req.shape, f32)

        @pl.when(jnp.logical_not(exists(axis, sign)))
        def _():
            for t in range(SWEEPS):
                drecv[t, d] = jnp.zeros((outer, pairs), f32)

    live = jnp.broadcast_to(live_ref[0], (blocks, pairs))
    live_rows = lax.broadcasted_iota(jnp.int32, (blocks, pairs), 0) < live
    lane_node = lax.broadcasted_iota(jnp.int32, (pairs, bz), 1).astype(f32)
    node_t = jnp.transpose(node_ref[0, 0, 0].astype(f32))
    for b in range(blocks):
        hot[pl.ds(b * pairs, pairs), :] = jnp.where(
            node_t[:, b : b + 1] == lane_node, 1.0, 0.0
        ).astype(bf16)
    row_line = line_ref[0, 0].astype(f32)
    two[...] = jnp.concatenate([row_line, row_line], axis=1)
    row_mod = lax.broadcasted_iota(jnp.int32, (blocks, blocks), 0)
    col_mod = lax.broadcasted_iota(jnp.int32, (blocks, blocks), 1)
    line_b = cols[0]
    same = line_b[:, :blocks] == row_line
    first_col = 1.0 - jnp.max(
        jnp.where(same & (col_mod < row_mod), 1.0, 0.0), axis=1, keepdims=True
    )

    def expand(stack, step):
        rows = stack.shape[0]
        which = lax.rem(lax.broadcasted_iota(jnp.int32, (rows, pairs), 0), step)
        return jnp.concatenate(
            [jnp.where(which == j, stack, 0.0).astype(bf16) for j in range(step)], axis=1
        )

    counts = []
    for g in range(blocks // 8):
        ones = jnp.where(live_rows[8 * g : 8 * g + 8], 1.0, 0.0)
        counts.append(mm(expand(ones, 8), hot[pl.ds(8 * g * pairs, 8 * pairs), :]))
    counts = jnp.concatenate(counts, axis=0).astype(bf16)

    def located(code, zpos, shift):
        e = jnp.floor((code + 0.5) / (by + 2 * RIM))
        f = code - e * (by + 2 * RIM)
        e = e - (RIM + shift[0] * bx)
        f = f - (RIM + shift[1] * by)
        z = zpos - (RIM + shift[2] * bz)
        ok_line = (e >= 0) & (e < bx) & (f >= 0) & (f < by)
        return jnp.where(ok_line, e * by + f, -1.0), z, ok_line & (z >= 0) & (z < bz)

    def setup(row, line, node, geom):
        n = line.shape[0]
        lane_line = lax.broadcasted_iota(jnp.int32, (n, lines), 1).astype(f32)
        a = jnp.where(line[:, : 2 * blocks] == two[...], 1.0, 0.0).astype(bf16)
        amat[pl.ds(row, n), :] = a
        cinv[pl.ds(row, n), :] = RELAX / (1.0 + mm(a[:, :blocks], counts))
        idx = node.astype(jnp.int32)
        low = lax.bitwise_and(idx, 127)
        half = lax.shift_right_logical(idx, 7)
        low_ref[pl.ds(row, n), :] = low
        half_ref[pl.ds(row, n), :] = half
        own = jnp.where(line == lane_line, 1.0, 0.0).astype(bf16)
        total = jnp.zeros((n, pairs), f32)
        for c in range(3):
            geo[c, pl.ds(row, n), :] = geom[c]
            vals = jnp.zeros((n, bz), f32)
            for part in split(pos_ref[c].reshape(lines, bz), 3):
                vals += mm(own, part)
            total += geom[c] * take_lanes(vals, low, half)
        return total

    def cat(parts):
        return jnp.concatenate(parts, axis=0)

    pos_copy.wait()
    for d, (axis, sign) in enumerate(dirs):

        @pl.when(exists(axis, -sign))
        def _():
            ask(d, axis, sign).wait_recv()

    asked = []
    for d, (axis, sign) in enumerate(dirs):
        shift = [0, 0, 0]
        shift[axis] = sign
        line, z, ok = located(reqs[d, 4], reqs[d, 3], shift)
        asked.append(
            [line, jnp.where(ok, z, 0.0)] + [jnp.where(ok, -reqs[d, c], 0.0) for c in range(3)]
        )
    asked = [cat([x[i] for x in asked]) for i in range(5)]
    base = asked[0].shape[0]
    rows = base + 2 * blocks

    def respond(t, total):
        for d, (axis, sign) in enumerate(dirs):
            dsend[t, d] = total[d * outer : (d + 1) * outer]
        for d, (axis, sign) in enumerate(dirs):

            @pl.when(exists(axis, -sign))
            def _():
                answer(t, d, axis, sign).start()

    def answer(t, d, axis, sign):
        return pltpu.make_async_remote_copy(
            src_ref=dsend.at[t, d],
            dst_ref=drecv.at[t, d],
            send_sem=ds_sem.at[t, d],
            recv_sem=dr_sem.at[t, d],
            device_id=neighbour(axis, -sign),
            device_id_type=MESH,
        )

    def received(t):
        for d, (axis, sign) in enumerate(dirs):

            @pl.when(exists(axis, sign))
            def _():
                answer(t, d, axis, sign).wait_recv()

        got = drecv[t, 0]
        for d in range(1, len(dirs)):
            got = got + drecv[t, d]
        return got

    respond(0, setup(0, asked[0], asked[1], asked[2:]))

    line, z, ok = located(cols[1], farpos_ref[0, 0, 0].astype(f32), (0, 0, 0))
    geom = [geom_ref[0, 0, 0, :, c, :] for c in range(4)]
    start = setup(
        base,
        cat([line_b, line]),
        cat([node_ref[0, 0, 0].astype(f32), jnp.where(ok, z, 0.0)]),
        [cat([geom[c], jnp.where(ok, -geom[c], 0.0)]) for c in range(3)],
    )
    start = start[:blocks] + start[blocks:] - geom[3]
    gap[0:outer, :] = start[:outer]
    gap[pl.ds(outer, outer), :] = start[outer:] + received(0)
    acc_ref[...] = jnp.zeros_like(acc_ref)

    def to_all(ref, send_sem, recv_sem):
        def send(k, carry):
            pltpu.make_async_remote_copy(
                src_ref=ref,
                dst_ref=ref,
                send_sem=send_sem,
                recv_sem=recv_sem,
                device_id=coords(k),
                device_id_type=MESH,
            ).start()
            return carry

        lax.fori_loop(1, devices, send, 0)

    def lanes_sum(x):
        x = jnp.sum(x, axis=0, keepdims=True)
        out = x[:, :128]
        for j in range(1, x.shape[1] // 128):
            out = out + x[:, 128 * j : 128 * (j + 1)]
        return out

    lane = lax.broadcasted_iota(jnp.int32, (1, 128), 1)

    def apply(row, n, parts):
        both = mm(amat[row : row + n, :], parts)
        return [both[:, c * bz : (c + 1) * bz] * cinv[row : row + n, :] for c in range(3)]

    def dots(row, n, moved):
        low = low_ref[row : row + n, :]
        half = half_ref[row : row + n, :]
        total = geo[0, row : row + n] * take_lanes(moved[0], low, half)
        for c in range(1, 3):
            total += geo[c, row : row + n] * take_lanes(moved[c], low, half)
        return total

    def sweep(t, last):
        depth = jnp.where(live_rows, jnp.maximum(-gap[...], 0.0), 0.0)
        squares = lanes_sum(depth * depth)
        if not last:
            erecv[t, mine] = squares
            to_all(erecv.at[t, mine], es_sem.at[t], er_sem.at[t])
        for g in range(blocks // 8):
            lo, hi = 8 * g, 8 * g + 8
            terms = cat([depth[lo:hi] * geo[c, base + lo : base + hi] for c in range(3)])
            top = terms.astype(bf16).astype(f32)
            sums = mm(expand(cat([top, terms - top]), 8), hot[pl.ds(lo * pairs, 8 * pairs), :])
            sums = sums[:24] + sums[24:]
            for c in range(3):
                wcat[lo:hi, c * bz : (c + 1) * bz] = sums[8 * c : 8 * c + 8]
        parts = cat(split(wcat[...], 2))
        if not last:
            respond(t + 1, dots(0, base, apply(0, base, parts)))
        moved = apply(base, blocks if last else 2 * blocks, parts)
        near = jnp.concatenate([m[:blocks] for m in moved], axis=1)
        resid = jnp.sum(lanes_sum(near * near * first_col), axis=1, keepdims=True)
        rrecv[mine] = jnp.where(lane == t, resid, rrecv[mine])
        if last:
            energy = jnp.sum(squares, axis=1, keepdims=True)
            rrecv[mine] = jnp.where(lane == SWEEPS, energy, rrecv[mine])
            to_all(rrecv.at[mine], rs_sem, rr_sem)
            others = rrecv.at[pl.ds(0, devices - 1)]
            pltpu.make_async_copy(others, others, rr_sem).wait()
            energy = jnp.sum(rrecv[...], axis=0)[:, SWEEPS : SWEEPS + 1]
        else:
            step = dots(base, 2 * blocks, moved)
            step = step[:blocks] + step[blocks:]
            others = erecv.at[t, pl.ds(0, devices - 1)]
            pltpu.make_async_copy(others, others, er_sem.at[t]).wait()
            energy = jnp.sum(jnp.sum(erecv[t], axis=0), axis=1, keepdims=True)
        scale = 1.0 / (1.0 + energy / (blocks * pairs * devices))
        hist_ref[0:1, :] = jnp.where(lane == t, energy, hist_ref[0:1, :])
        hist_ref[1:2, :] = jnp.where(lane == t, scale, hist_ref[1:2, :])
        acc_ref[...] = acc_ref[...] + (scale * first_col) * near
        if not last:
            more = received(t + 1)
            gap[0:outer, :] = gap[0:outer, :] + scale * step[:outer]
            gap[pl.ds(outer, outer), :] = gap[pl.ds(outer, outer), :] + scale * (
                step[outer:] + more
            )

    rrecv[mine] = jnp.zeros((1, 128), f32)
    hist_ref[...] = jnp.zeros_like(hist_ref)

    def body(t, carry):
        sweep(t, False)
        return carry

    lax.fori_loop(0, SWEEPS - 1, body, 0)
    sweep(SWEEPS - 1, True)

    for d, (axis, sign) in enumerate(dirs):

        @pl.when(exists(axis, sign))
        def _():
            ask(d, axis, sign).wait_send()

        @pl.when(exists(axis, -sign))
        def _():
            for t in range(SWEEPS):
                answer(t, d, axis, sign).wait_send()

    for t in range(SWEEPS - 1):
        ref = erecv.at[t, pl.ds(0, devices - 1)]
        pltpu.make_async_copy(ref, ref, es_sem.at[t]).wait()
    others = rrecv.at[pl.ds(0, devices - 1)]
    pltpu.make_async_copy(others, others, rs_sem).wait()
    energy, scale = hist_ref[0:1, :], hist_ref[1:2, :]
    resid = jnp.sum(rrecv[...], axis=0)
    hist_ref[0:1, :] = jnp.sqrt(1.0 + energy / (blocks * pairs))
    hist_ref[1:2, :] = jnp.sqrt(1.0 + scale * scale * resid / (bx * by * bz))


def finish(acc_ref, line_ref, hist_in, pos_ref, out_ref, hist_ref):
    _, bx, by, bz = pos_ref.shape
    lines = bx * by
    row = line_ref[0, 0].astype(f32)
    row = jnp.concatenate([row, row], axis=1)
    rows = lax.broadcasted_iota(jnp.int32, (lines, row.shape[1]), 0).astype(f32)
    place = jnp.where(rows == row, 1.0, 0.0).astype(bf16)
    total = mm(place, jnp.concatenate(split(acc_ref[...], 2), axis=0))
    out_ref[0] = pos_ref[0] + total.reshape(bx, by, bz)
    hist_ref[...] = hist_in[0:2, : hist_ref.shape[1]]


def local(sizes, positions, pair_node, pair_line, pair_far, far_line, pair_geom, live_blocks):
    blocks, pairs = pair_node.shape[3:]
    blk = positions.shape[1:]
    devices = sizes[0] * sizes[1] * sizes[2]
    outer = blocks // 2
    rows = 2 * blocks + 6 * outer
    dma = pltpu.SemaphoreType.DMA
    vmem = pl.BlockSpec(memory_space=pltpu.VMEM)
    moved, hist = pl.pallas_call(
        functools.partial(kernel, sizes, blk),
        out_shape=(
            jax.ShapeDtypeStruct((blocks, 3 * blk[2]), f32),
            jax.ShapeDtypeStruct((8, 128), f32),
        ),
        in_specs=[vmem] * 6 + [pl.BlockSpec(memory_space=pl.ANY)],
        out_specs=(vmem, vmem),
        scratch_shapes=[
            pltpu.VMEM(positions.shape, f32),
            pltpu.VMEM((5, outer, pairs), f32),
            pltpu.VMEM((2, blocks, pairs), f32),
            pltpu.VMEM((blocks * pairs, blk[2]), bf16),
            pltpu.VMEM((1, 2 * blocks), f32),
            pltpu.VMEM((rows, 2 * blocks), bf16),
            pltpu.VMEM((rows, pairs), f32),
            pltpu.VMEM((3, rows, pairs), f32),
            pltpu.VMEM((rows, pairs), jnp.int32),
            pltpu.VMEM((rows, pairs), jnp.int32),
            pltpu.VMEM((blocks, pairs), f32),
            pltpu.VMEM((blocks, 3 * blk[2]), f32),
            pltpu.VMEM((6, 5, outer, pairs), f32),
            pltpu.VMEM((SWEEPS, 6, outer, pairs), f32),
            pltpu.VMEM((SWEEPS, 6, outer, pairs), f32),
            pltpu.VMEM((SWEEPS, devices, 1, 128), f32),
            pltpu.VMEM((devices, 1, 128), f32),
            dma,
            dma((6,)),
            dma((6,)),
            dma((SWEEPS, 6)),
            dma((SWEEPS, 6)),
            dma((SWEEPS,)),
            dma((SWEEPS,)),
            dma,
            dma,
        ],
        compiler_params=pltpu.CompilerParams(has_side_effects=True),
    )(live_blocks, pair_node, pair_line, pair_far, far_line, pair_geom, positions)
    return pl.pallas_call(
        finish,
        grid=(3,),
        out_shape=(
            jax.ShapeDtypeStruct(positions.shape, f32),
            jax.ShapeDtypeStruct((2, SWEEPS), f32),
        ),
        in_specs=[
            pl.BlockSpec((blocks, blk[2]), lambda c: (0, c)),
            pl.BlockSpec(pair_line.shape, lambda c: (0, 0, 0, 0)),
            pl.BlockSpec((8, 128), lambda c: (0, 0)),
            pl.BlockSpec((1,) + blk, lambda c: (c, 0, 0, 0)),
        ],
        out_specs=(
            pl.BlockSpec((1,) + blk, lambda c: (c, 0, 0, 0)),
            pl.BlockSpec((2, SWEEPS), lambda c: (0, 0)),
        ),
    )(moved, pair_line, hist, positions)


def solution(mesh):
    sizes = tuple(mesh.shape[a] for a in AXES)
    return jax.shard_map(
        functools.partial(local, sizes),
        mesh=mesh,
        in_specs=(
            P(None, "gx", "gy", "gz"),
            P("gx", "gy", "gz", None, None),
            P("gx", "gy", "gz", None),
            P("gx", "gy", "gz", None, None),
            P("gx", "gy", "gz", None),
            P("gx", "gy", "gz", None, None, None),
            P("gx", "gy", "gz"),
        ),
        out_specs=(P(None, "gx", "gy", "gz"), P()),
        check_vma=False,
    )
```

```python
import functools

import jax
import jax.numpy as jnp
from jax import lax
from jax.experimental import pallas as pl
from jax.experimental.pallas import tpu as pltpu
from jax.sharding import PartitionSpec as P

RIM = 3
SWEEPS = 5
RELAX = 0.9
AXES = ("gx", "gy", "gz")
MESH = pl.DeviceIdType.MESH
f32 = jnp.float32
bf16 = jnp.bfloat16


def split(x, parts):
    out = []
    for _ in range(parts - 1):
        hi = x.astype(bf16)
        out.append(hi)
        x = x - hi.astype(f32)
    out.append(x.astype(bf16))
    return out


def mm(a, b):
    return jnp.dot(a, b, preferred_element_type=f32)


def take_lanes(x, low, half):
    outs = []
    for h in range(0, low.shape[1], 128):
        idx = low[:, h : h + 128]
        got = jnp.take_along_axis(x[:, :128], idx, axis=1, mode="promise_in_bounds")
        for j in range(1, x.shape[1] // 128):
            more = jnp.take_along_axis(
                x[:, 128 * j : 128 * (j + 1)], idx, axis=1, mode="promise_in_bounds"
            )
            got = jnp.where(half[:, h : h + 128] == j, more, got)
        outs.append(got)
    return jnp.concatenate(outs, axis=1)


def kernel(
    sizes,
    blk,
    live_ref,
    node_ref,
    line_ref,
    farpos_ref,
    farline_ref,
    geom_ref,
    pos_hbm,
    acc_ref,
    hist_ref,
    pos_ref,
    req,
    cols,
    hot,
    two,
    amat,
    cinv,
    geo,
    low_ref,
    half_ref,
    gap,
    wcat,
    reqs,
    dsend,
    drecv,
    erecv,
    rrecv,
    pos_sem,
    qs_sem,
    qr_sem,
    ds_sem,
    dr_sem,
    es_sem,
    er_sem,
    rs_sem,
    rr_sem,
):
    nx, ny, nz = sizes
    bx, by, bz = blk
    devices = nx * ny * nz
    blocks, pairs = gap.shape
    outer = blocks // 2
    lines = bx * by
    me = [lax.axis_index(a) for a in AXES]
    mine = (me[0] * ny + me[1]) * nz + me[2]
    dirs = [(a, s) for a in (1, 0, 2) for s in (1, -1)]

    def neighbour(axis, sign):
        to = list(me)
        to[axis] = lax.rem(me[axis] + sign + sizes[axis], sizes[axis])
        return tuple(to)

    def exists(axis, sign):
        return (me[axis] + sign >= 0) & (me[axis] + sign < sizes[axis])

    def coords(k):
        to = lax.rem(mine + k, devices)
        return (to // (ny * nz), lax.rem(to // nz, ny), lax.rem(to, nz))

    pos_copy = pltpu.make_async_copy(pos_hbm, pos_ref, pos_sem)
    pos_copy.start()

    def column(ref):
        row = ref[0, 0].astype(f32)
        return jnp.transpose(jnp.broadcast_to(row, (pairs, blocks)))

    wide = pairs // 128
    planes = [geom_ref[0, 0, 0, outer:, c, :] for c in range(3)]
    planes.append(farpos_ref[0, 0, 0, outer:, :].astype(f32))
    for c in range(4):
        for h in range(wide):
            req[c * wide + h] = planes[c][:, 128 * h : 128 * (h + 1)]
    cols[1] = column(farline_ref)
    req[4 * wide] = cols[1, outer:, :128]
    cols[0] = column(line_ref)
    def ask(d, axis, sign):
        return pltpu.make_async_remote_copy(
            src_ref=req,
            dst_ref=reqs.at[d],
            send_sem=qs_sem.at[d],
            recv_sem=qr_sem.at[d],
            device_id=neighbour(axis, sign),
            device_id_type=MESH,
        )

    for d, (axis, sign) in enumerate(dirs):

        @pl.when(exists(axis, sign))
        def _():
            ask(d, axis, sign).start()

    for d, (axis, sign) in enumerate(dirs):

        @pl.when(jnp.logical_not(exists(axis, -sign)))
        def _():
            reqs[d] = jnp.zeros(req.shape, f32)

        @pl.when(jnp.logical_not(exists(axis, sign)))
        def _():
            for t in range(SWEEPS):
                drecv[t, d] = jnp.zeros((outer, pairs), f32)

    live = jnp.broadcast_to(live_ref[0], (blocks, pairs))
    live_rows = lax.broadcasted_iota(jnp.int32, (blocks, pairs), 0) < live
    lane_node = lax.broadcasted_iota(jnp.int32, (pairs, bz), 1).astype(f32)
    node_t = jnp.transpose(node_ref[0, 0, 0].astype(f32))
    for b in range(blocks):
        hot[pl.ds(b * pairs, pairs), :] = jnp.where(
            node_t[:, b : b + 1] == lane_node, 1.0, 0.0
        ).astype(bf16)
    row_line = line_ref[0, 0].astype(f32)
    two[...] = jnp.concatenate([row_line, row_line], axis=1)
    row_mod = lax.broadcasted_iota(jnp.int32, (blocks, blocks), 0)
    col_mod = lax.broadcasted_iota(jnp.int32, (blocks, blocks), 1)
    line_b = cols[0]
    same = line_b[:, :blocks] == row_line
    first_col = 1.0 - jnp.max(
        jnp.where(same & (col_mod < row_mod), 1.0, 0.0), axis=1, keepdims=True
    )

    def expand(stack, step):
        rows = stack.shape[0]
        which = lax.rem(lax.broadcasted_iota(jnp.int32, (rows, pairs), 0), step)
        return jnp.concatenate(
            [jnp.where(which == j, stack, 0.0).astype(bf16) for j in range(step)], axis=1
        )

    counts = []
    for g in range(blocks // 8):
        ones = jnp.where(live_rows[8 * g : 8 * g + 8], 1.0, 0.0)
        counts.append(mm(expand(ones, 8), hot[pl.ds(8 * g * pairs, 8 * pairs), :]))
    counts = jnp.concatenate(counts, axis=0).astype(bf16)

    def located(code, zpos, shift):
        e = jnp.floor((code + 0.5) / (by + 2 * RIM))
        f = code - e * (by + 2 * RIM)
        e = e - (RIM + shift[0] * bx)
        f = f - (RIM + shift[1] * by)
        z = zpos - (RIM + shift[2] * bz)
        ok_line = (e >= 0) & (e < bx) & (f >= 0) & (f < by)
        return jnp.where(ok_line, e * by + f, -1.0), z, ok_line & (z >= 0) & (z < bz)

    def setup(row, line, node, geom):
        n = line.shape[0]
        lane_line = lax.broadcasted_iota(jnp.int32, (n, lines), 1).astype(f32)
        a = jnp.where(line[:, : 2 * blocks] == two[...], 1.0, 0.0).astype(bf16)
        amat[pl.ds(row, n), :] = a
        cinv[pl.ds(row, n), :] = RELAX / (1.0 + mm(a[:, :blocks], counts))
        idx = node.astype(jnp.int32)
        low = lax.bitwise_and(idx, 127)
        half = lax.shift_right_logical(idx, 7)
        low_ref[pl.ds(row, n), :] = low
        half_ref[pl.ds(row, n), :] = half
        own = jnp.where(line == lane_line, 1.0, 0.0).astype(bf16)
        total = jnp.zeros((n, pairs), f32)
        for c in range(3):
            geo[c, pl.ds(row, n), :] = geom[c]
            vals = jnp.zeros((n, bz), f32)
            for part in split(pos_ref[c].reshape(lines, bz), 3):
                vals += mm(own, part)
            total += geom[c] * take_lanes(vals, low, half)
        return total

    def cat(parts):
        return jnp.concatenate(parts, axis=0)

    pos_copy.wait()
    for d, (axis, sign) in enumerate(dirs):

        @pl.when(exists(axis, -sign))
        def _():
            ask(d, axis, sign).wait_recv()

    asked = []
    for d, (axis, sign) in enumerate(dirs):
        shift = [0, 0, 0]
        shift[axis] = sign
        got = [
            jnp.concatenate([reqs[d, c * wide + h] for h in range(wide)], axis=1) for c in range(4)
        ]
        code = jnp.concatenate([reqs[d, 4 * wide]] * wide, axis=1)
        line, z, ok = located(code, got[3], shift)
        asked.append(
            [line, jnp.where(ok, z, 0.0)] + [jnp.where(ok, -got[c], 0.0) for c in range(3)]
        )
    asked = [cat([x[i] for x in asked]) for i in range(5)]
    base = asked[0].shape[0]
    rows = base + 2 * blocks

    def respond(t, total):
        for d, (axis, sign) in enumerate(dirs):
            dsend[t, d] = total[d * outer : (d + 1) * outer]
        for d, (axis, sign) in enumerate(dirs):

            @pl.when(exists(axis, -sign))
            def _():
                answer(t, d, axis, sign).start()

    def answer(t, d, axis, sign):
        return pltpu.make_async_remote_copy(
            src_ref=dsend.at[t, d],
            dst_ref=drecv.at[t, d],
            send_sem=ds_sem.at[t, d],
            recv_sem=dr_sem.at[t, d],
            device_id=neighbour(axis, -sign),
            device_id_type=MESH,
        )

    def received(t):
        for d, (axis, sign) in enumerate(dirs):

            @pl.when(exists(axis, sign))
            def _():
                answer(t, d, axis, sign).wait_recv()

        got = drecv[t, 0]
        for d in range(1, len(dirs)):
            got = got + drecv[t, d]
        return got

    respond(0, setup(0, asked[0], asked[1], asked[2:]))

    line, z, ok = located(cols[1], farpos_ref[0, 0, 0].astype(f32), (0, 0, 0))
    geom = [geom_ref[0, 0, 0, :, c, :] for c in range(4)]
    start = setup(
        base,
        cat([line_b, line]),
        cat([node_ref[0, 0, 0].astype(f32), jnp.where(ok, z, 0.0)]),
        [cat([geom[c], jnp.where(ok, -geom[c], 0.0)]) for c in range(3)],
    )
    start = start[:blocks] + start[blocks:] - geom[3]
    gap[0:outer, :] = start[:outer]
    gap[pl.ds(outer, outer), :] = start[outer:] + received(0)
    acc_ref[...] = jnp.zeros_like(acc_ref)

    def to_all(ref, send_sem, recv_sem):
        def send(k, carry):
            pltpu.make_async_remote_copy(
                src_ref=ref,
                dst_ref=ref,
                send_sem=send_sem,
                recv_sem=recv_sem,
                device_id=coords(k),
                device_id_type=MESH,
            ).start()
            return carry

        lax.fori_loop(1, devices, send, 0, unroll=devices <= 32)

    def lanes_sum(x):
        x = jnp.sum(x, axis=0, keepdims=True)
        out = x[:, :128]
        for j in range(1, x.shape[1] // 128):
            out = out + x[:, 128 * j : 128 * (j + 1)]
        return out

    lane = lax.broadcasted_iota(jnp.int32, (1, 128), 1)

    def apply(row, n, parts):
        both = mm(amat[row : row + n, :], parts)
        return [both[:, c * bz : (c + 1) * bz] * cinv[row : row + n, :] for c in range(3)]

    def dots(row, n, moved):
        low = low_ref[row : row + n, :]
        half = half_ref[row : row + n, :]
        total = geo[0, row : row + n] * take_lanes(moved[0], low, half)
        for c in range(1, 3):
            total += geo[c, row : row + n] * take_lanes(moved[c], low, half)
        return total

    def sweep(t, last):
        depth = jnp.where(live_rows, jnp.maximum(-gap[...], 0.0), 0.0)
        squares = lanes_sum(depth * depth)
        if not last:
            erecv[t, mine] = squares
            to_all(erecv.at[t, mine], es_sem.at[t], er_sem.at[t])
        for g in range(blocks // 8):
            lo, hi = 8 * g, 8 * g + 8
            terms = cat([depth[lo:hi] * geo[c, base + lo : base + hi] for c in range(3)])
            top = terms.astype(bf16).astype(f32)
            sums = mm(expand(cat([top, terms - top]), 8), hot[pl.ds(lo * pairs, 8 * pairs), :])
            sums = sums[:24] + sums[24:]
            for c in range(3):
                wcat[lo:hi, c * bz : (c + 1) * bz] = sums[8 * c : 8 * c + 8]
        parts = cat(split(wcat[...], 2))
        if not last:
            respond(t + 1, dots(0, base, apply(0, base, parts)))
        moved = apply(base, blocks if last else 2 * blocks, parts)
        near = jnp.concatenate([m[:blocks] for m in moved], axis=1)
        resid = jnp.sum(lanes_sum(near * near * first_col), axis=1, keepdims=True)
        rrecv[mine] = jnp.where(lane == t, resid, rrecv[mine])
        if last:
            energy = jnp.sum(squares, axis=1, keepdims=True)
            rrecv[mine] = jnp.where(lane == SWEEPS, energy, rrecv[mine])
            to_all(rrecv.at[mine], rs_sem, rr_sem)
            others = rrecv.at[pl.ds(0, devices - 1)]
            pltpu.make_async_copy(others, others, rr_sem).wait()
            energy = jnp.sum(rrecv[...], axis=0)[:, SWEEPS : SWEEPS + 1]
        else:
            step = dots(base, 2 * blocks, moved)
            step = step[:blocks] + step[blocks:]
            others = erecv.at[t, pl.ds(0, devices - 1)]
            pltpu.make_async_copy(others, others, er_sem.at[t]).wait()
            energy = jnp.sum(jnp.sum(erecv[t], axis=0), axis=1, keepdims=True)
        scale = 1.0 / (1.0 + energy / (blocks * pairs * devices))
        hist_ref[0:1, :] = jnp.where(lane == t, energy, hist_ref[0:1, :])
        hist_ref[1:2, :] = jnp.where(lane == t, scale, hist_ref[1:2, :])
        acc_ref[...] = acc_ref[...] + (scale * first_col) * near
        if not last:
            more = received(t + 1)
            gap[0:outer, :] = gap[0:outer, :] + scale * step[:outer]
            gap[pl.ds(outer, outer), :] = gap[pl.ds(outer, outer), :] + scale * (
                step[outer:] + more
            )

    rrecv[mine] = jnp.zeros((1, 128), f32)
    hist_ref[...] = jnp.zeros_like(hist_ref)

    def body(t, carry):
        sweep(t, False)
        return carry

    lax.fori_loop(0, SWEEPS - 1, body, 0)
    sweep(SWEEPS - 1, True)

    for d, (axis, sign) in enumerate(dirs):

        @pl.when(exists(axis, sign))
        def _():
            ask(d, axis, sign).wait_send()

        @pl.when(exists(axis, -sign))
        def _():
            for t in range(SWEEPS):
                answer(t, d, axis, sign).wait_send()

    for t in range(SWEEPS - 1):
        ref = erecv.at[t, pl.ds(0, devices - 1)]
        pltpu.make_async_copy(ref, ref, es_sem.at[t]).wait()
    others = rrecv.at[pl.ds(0, devices - 1)]
    pltpu.make_async_copy(others, others, rs_sem).wait()
    energy, scale = hist_ref[0:1, :], hist_ref[1:2, :]
    resid = jnp.sum(rrecv[...], axis=0)
    hist_ref[0:1, :] = jnp.sqrt(1.0 + energy / (blocks * pairs))
    hist_ref[1:2, :] = jnp.sqrt(1.0 + scale * scale * resid / (bx * by * bz))


def finish(acc_ref, line_ref, hist_in, pos_ref, out_ref, hist_ref):
    _, bx, by, bz = pos_ref.shape
    lines = bx * by
    row = line_ref[0, 0].astype(f32)
    row = jnp.concatenate([row, row], axis=1)
    rows = lax.broadcasted_iota(jnp.int32, (lines, row.shape[1]), 0).astype(f32)
    place = jnp.where(rows == row, 1.0, 0.0).astype(bf16)
    total = mm(place, jnp.concatenate(split(acc_ref[...], 2), axis=0))
    out_ref[0] = pos_ref[0] + total.reshape(bx, by, bz)
    hist_ref[...] = hist_in[0:2, : hist_ref.shape[1]]


def local(sizes, positions, pair_node, pair_line, pair_far, far_line, pair_geom, live_blocks):
    blocks, pairs = pair_node.shape[3:]
    blk = positions.shape[1:]
    devices = sizes[0] * sizes[1] * sizes[2]
    outer = blocks // 2
    rows = 2 * blocks + 6 * outer
    dma = pltpu.SemaphoreType.DMA
    vmem = pl.BlockSpec(memory_space=pltpu.VMEM)
    moved, hist = pl.pallas_call(
        functools.partial(kernel, sizes, blk),
        out_shape=(
            jax.ShapeDtypeStruct((blocks, 3 * blk[2]), f32),
            jax.ShapeDtypeStruct((8, 128), f32),
        ),
        in_specs=[vmem] * 6 + [pl.BlockSpec(memory_space=pl.ANY)],
        out_specs=(vmem, vmem),
        scratch_shapes=[
            pltpu.VMEM(positions.shape, f32),
            pltpu.VMEM((4 * (pairs // 128) + 1, outer, 128), f32),
            pltpu.VMEM((2, blocks, pairs), f32),
            pltpu.VMEM((blocks * pairs, blk[2]), bf16),
            pltpu.VMEM((1, 2 * blocks), f32),
            pltpu.VMEM((rows, 2 * blocks), bf16),
            pltpu.VMEM((rows, pairs), f32),
            pltpu.VMEM((3, rows, pairs), f32),
            pltpu.VMEM((rows, pairs), jnp.int32),
            pltpu.VMEM((rows, pairs), jnp.int32),
            pltpu.VMEM((blocks, pairs), f32),
            pltpu.VMEM((blocks, 3 * blk[2]), f32),
            pltpu.VMEM((6, 4 * (pairs // 128) + 1, outer, 128), f32),
            pltpu.VMEM((SWEEPS, 6, outer, pairs), f32),
            pltpu.VMEM((SWEEPS, 6, outer, pairs), f32),
            pltpu.VMEM((SWEEPS, devices, 1, 128), f32),
            pltpu.VMEM((devices, 1, 128), f32),
            dma,
            dma((6,)),
            dma((6,)),
            dma((SWEEPS, 6)),
            dma((SWEEPS, 6)),
            dma((SWEEPS,)),
            dma((SWEEPS,)),
            dma,
            dma,
        ],
        compiler_params=pltpu.CompilerParams(has_side_effects=True),
    )(live_blocks, pair_node, pair_line, pair_far, far_line, pair_geom, positions)
    return pl.pallas_call(
        finish,
        grid=(3,),
        out_shape=(
            jax.ShapeDtypeStruct(positions.shape, f32),
            jax.ShapeDtypeStruct((2, SWEEPS), f32),
        ),
        in_specs=[
            pl.BlockSpec((blocks, blk[2]), lambda c: (0, c)),
            pl.BlockSpec(pair_line.shape, lambda c: (0, 0, 0, 0)),
            pl.BlockSpec((8, 128), lambda c: (0, 0)),
            pl.BlockSpec((1,) + blk, lambda c: (c, 0, 0, 0)),
        ],
        out_specs=(
            pl.BlockSpec((1,) + blk, lambda c: (c, 0, 0, 0)),
            pl.BlockSpec((2, SWEEPS), lambda c: (0, 0)),
        ),
    )(moved, pair_line, hist, positions)


def solution(mesh):
    sizes = tuple(mesh.shape[a] for a in AXES)
    return jax.shard_map(
        functools.partial(local, sizes),
        mesh=mesh,
        in_specs=(
            P(None, "gx", "gy", "gz"),
            P("gx", "gy", "gz", None, None),
            P("gx", "gy", "gz", None),
            P("gx", "gy", "gz", None, None),
            P("gx", "gy", "gz", None),
            P("gx", "gy", "gz", None, None, None),
            P("gx", "gy", "gz"),
        ),
        out_specs=(P(None, "gx", "gy", "gz"), P()),
        check_vma=False,
    )
```
